256 devices in a mesh: groups: 2 (over z), seq: 128 (over x, y, core).
Axes of the slice: x: 8, y: 8, z: 2, core: 2. Of those that a mesh axis runs over, the one named last changes fastest.
The devices are a block of a 8x8x16 slice.
Arguments:
- query_rows: bfloat16 [131072, 1536], P(('groups', 'seq')), parts along dimension 0, may hold values from -200 to 200
- key_rows: bfloat16 [131072, 1536], P(('groups', 'seq')), parts along dimension 0, may hold values from -6 to 6
- value_rows: bfloat16 [131072, 1536], P(('groups', 'seq')), parts along dimension 0, may hold values from -6 to 6
- select: int32 [512, 6], P('groups'), parts along dimension 0, may hold values from 0 to 255, as said below
- counts: int32 [512], P('groups'), parts along dimension 0, may hold values from 2 to 6, as said below
- guide_scale: float32 [2], P('groups'), parts along dimension 0, may hold values from 4 to 8
Outputs:
- guided: bfloat16 [65536, 1536], P(('groups', 'seq')), parts along dimension 0
The draws below stay inside these ranges and needn't reach their ends.
There are 2 independent parts, one for each index of `groups`. The reference program is written for one: setup_inputs(seed, part) draws one part's arguments, and reference() takes and returns one part's arrays. A program takes and returns all parts, laid end to end along the dimension named above; each array names one. Nothing has to cross between parts.
Inputs may be any that keep to these rules, and one draw needn't show every extreme that they name: Row i begins with i itself. Its first counts[i] entries are distinct and name tiles of shards within 2 of tile i's shard, where tile t belongs to shard t // 4. The query tiles of one shard select at most 2 distinct tiles of any one other shard, and every shard selects 2 tiles of each shard within 2 in every draw. Entries past counts[i] are valid tile numbers that are not used. `counts`: whole shards are heavy or light, so the work of one device differs by about two times between devices.
All inputs are finite; a program needn't handle non-finite values.
Results may differ from the reference program's by a relative error of at most 0.0075.
Values may be sent and summed in bfloat16 or wider, within the bound.
A program may use at most 128 MiB of HBM per device.

```python
import jax
import jax.numpy as jnp
from jax import lax

HEADS = 12
HEAD_DIM = 128
TILE = 128
TOK_DEV = 512
REACH = 2
CAP = 2
PICKS = 6
WIDTH = 1536
TILES_DEV = 4
SHARDS = 64
SEQLEN = 32768
NTILES = 256


def mask_tables(key):
    folded = jax.random.fold_in(key, 101)
    key_pool, key_score, key_heavy, key_count = jax.random.split(folded, 4)
    cand_count = TILES_DEV + 2 * REACH * CAP
    offset_list = jnp.array([moved for moved in range(-REACH, REACH + 1) if moved != 0], dtype=jnp.int32)
    shard_ids = jnp.arange(SHARDS, dtype=jnp.int32)
    tile_ids = jnp.arange(TILES_DEV, dtype=jnp.int32)
    pool_scores = jax.random.randint(key_pool, (SHARDS, 2 * REACH, TILES_DEV), 0, 1 << 16, dtype=jnp.int32) * TILES_DEV + tile_ids
    pool_local = lax.top_k(pool_scores, CAP)[1].astype(jnp.int32)
    owner_ids = shard_ids[:, None, None] + offset_list[None, :, None]
    pool_tiles = owner_ids * TILES_DEV + pool_local
    pool_valid = jnp.broadcast_to((owner_ids >= 0) & (owner_ids < SHARDS), pool_local.shape)
    local_tiles = shard_ids[:, None] * TILES_DEV + tile_ids[None, :]
    candidates = jnp.concatenate([local_tiles, pool_tiles.reshape(SHARDS, 2 * REACH * CAP)], axis=1)
    cand_valid = jnp.concatenate([jnp.ones((SHARDS, TILES_DEV), dtype=bool), pool_valid.reshape(SHARDS, 2 * REACH * CAP)], axis=1)
    cand_index = jnp.arange(cand_count, dtype=jnp.int32)
    noise_scores = jax.random.randint(key_score, (SHARDS, TILES_DEV, cand_count), 0, 1 << 16, dtype=jnp.int32) * cand_count + cand_index
    self_slot = cand_index[None, :] == tile_ids[:, None]
    block_index = (cand_index - TILES_DEV) // CAP
    row_of_block = (shard_ids[:, None] + block_index[None, :]) % TILES_DEV
    in_forced = (cand_index >= TILES_DEV)[None, None, :] & (tile_ids[None, :, None] == row_of_block[:, None, :])
    total_score = noise_scores + jnp.where(self_slot[None, :, :], 1 << 26, 0) + jnp.where(in_forced, 1 << 24, 0) - jnp.where(cand_valid[:, None, :], 0, 1 << 27)
    best_index = lax.top_k(total_score, PICKS)[1].astype(jnp.int32)
    spread = jnp.broadcast_to(candidates[:, None, :], (SHARDS, TILES_DEV, cand_count))
    select = jnp.take_along_axis(spread, best_index, axis=2).reshape(NTILES, PICKS).astype(jnp.int32)
    heavy_shard = jax.random.randint(key_heavy, (SHARDS,), 0, 4, dtype=jnp.int32) == 0
    many_picks = jax.random.randint(key_count, (SHARDS, TILES_DEV), PICKS - 2, PICKS + 1, dtype=jnp.int32)
    few_picks = jax.random.randint(jax.random.fold_in(key_count, 3), (SHARDS, TILES_DEV), 2, 4, dtype=jnp.int32)
    counts = jnp.where(heavy_shard[:, None], many_picks, few_picks)
    forced_row = (tile_ids[None, :] - shard_ids[:, None]) % TILES_DEV < 2 * REACH
    counts = jnp.where(forced_row, jnp.maximum(counts, CAP + 1), counts).reshape(NTILES).astype(jnp.int32)
    return (select, counts)


def draw_select(key, part):
    return mask_tables(key)[0]


def draw_counts(key, part):
    return mask_tables(key)[1]


def query_key_tables(key):
    folded = jax.random.fold_in(key, 202)
    key_query, key_key = jax.random.split(folded, 2)
    queries = jax.random.normal(key_query, (2 * SEQLEN, HEADS, HEAD_DIM), jnp.float32)
    keyset = jnp.clip(jax.random.normal(key_key, (2 * SEQLEN, HEADS, HEAD_DIM), jnp.float32), -6.0, 6.0)
    queries = jnp.clip(queries, -200.0, 200.0)
    return (queries.reshape(2 * SEQLEN, HEADS * HEAD_DIM), keyset.reshape(2 * SEQLEN, HEADS * HEAD_DIM))


def draw_query_rows(key, part):
    return query_key_tables(key)[0].astype(jnp.bfloat16)


def draw_key_rows(key, part):
    return query_key_tables(key)[1].astype(jnp.bfloat16)


def shard_levels(own_key, dims, cuts, low, largest):
    def one(dim, shards_of):
        draws = jax.random.uniform(jax.random.fold_in(jax.random.fold_in(own_key, 6), dim), (shards_of,), jnp.float32, low / len(cuts), largest / len(cuts))
        return jnp.repeat(jnp.exp(draws), dims[dim] // shards_of).reshape((-1,) + (1,) * (len(dims) - dim - 1))

    factor_of = one(*cuts[0])
    for cut in cuts[1:]:
        factor_of = factor_of * one(*cut)
    return factor_of


def scatter_about(own_key, dims, deviation, most, shards=(), kind=jnp.bfloat16):
    drawn = deviation * jax.random.normal(own_key, dims, jnp.float32)
    if shards:
        drawn = drawn * shard_levels(own_key, dims, shards, -0.22, 0.18)
    return jnp.clip(drawn, -most, most).astype(kind)


def setup_inputs(seed: int = 0, part: int = 0) -> dict:
    splits = jax.random.split(jax.random.key(seed), 7)
    own_keys = jax.random.split(jax.random.fold_in(splits[6], part), 7)
    query_rows = draw_query_rows(jax.random.fold_in(jax.random.fold_in(splits[6], part), 71), part)
    key_rows = draw_key_rows(jax.random.fold_in(jax.random.fold_in(splits[6], part), 71), part)
    value_rows = scatter_about(own_keys[2], (2 * SEQLEN, WIDTH), 1.0, 6.0, ((0, 128),))
    select = draw_select(jax.random.fold_in(jax.random.fold_in(splits[6], part), 71), part)
    counts = draw_counts(jax.random.fold_in(jax.random.fold_in(splits[6], part), 71), part)
    guide_scale = jnp.clip(jax.random.uniform(own_keys[5], (1,), jnp.float32, 4.0, 8.0), 4.0, 8.0)
    return {"query_rows": query_rows, "key_rows": key_rows, "value_rows": value_rows, "select": select, "counts": counts, "guide_scale": guide_scale}


def attend_tile(query_tile, key_sel, value_sel, alive_slots):
    score_scale = HEAD_DIM ** -0.5
    scores = jnp.einsum("thd,pshd->htps", query_tile.astype(jnp.float32), key_sel.astype(jnp.float32)) * score_scale
    scores = jnp.where(alive_slots[None, None, :, None], scores, -jnp.inf)
    row_max = jnp.max(scores, axis=(2, 3), keepdims=True)
    weights = jnp.exp(scores - row_max)
    denominator = jnp.sum(weights, axis=(2, 3))
    rounded = lax.optimization_barrier(weights.astype(jnp.bfloat16)).astype(jnp.float32)
    weighted = jnp.einsum("htps,pshd->thd", rounded, value_sel.astype(jnp.float32))
    return (weighted / jnp.transpose(denominator)[:, :, None]).astype(jnp.bfloat16)


def branch_major(rows, ntiles):
    split = rows.reshape(SHARDS, 2, TOK_DEV, HEADS * HEAD_DIM)
    return jnp.transpose(split, (1, 0, 2, 3)).reshape(2, ntiles, TILE, HEADS, HEAD_DIM)


def reference(query_rows, key_rows, value_rows, select, counts, guide_scale):
    ntiles = select.shape[0]
    query_tiles = branch_major(query_rows, ntiles)
    key_tiles = branch_major(key_rows, ntiles)
    value_tiles = branch_major(value_rows, ntiles)
    alive_all = jnp.arange(PICKS, dtype=jnp.int32)[None, :] < counts[:, None]
    guidance = guide_scale[0]

    def one_tile(inputs):
        cond_query, uncond_query, chosen, alive_slots = inputs
        cond_out = attend_tile(cond_query, key_tiles[0][chosen], value_tiles[0][chosen], alive_slots)
        uncond = attend_tile(uncond_query, key_tiles[1][chosen], value_tiles[1][chosen], alive_slots)
        cond_wide = lax.optimization_barrier(cond_out).astype(jnp.float32)
        uncond_wide = lax.optimization_barrier(uncond).astype(jnp.float32)
        mixed_out = uncond_wide + guidance * (cond_wide - uncond_wide)
        return mixed_out.astype(jnp.bfloat16).reshape(TILE, HEADS * HEAD_DIM)

    guided = lax.map(one_tile, (query_tiles[0], query_tiles[1], select, alive_all), batch_size=4)
    return guided.reshape(ntiles * TILE, HEADS * HEAD_DIM)
```

```python
import jax
import jax.numpy as jnp
from jax import lax
from jax.experimental import pallas as pl
from jax.experimental.pallas import tpu as pltpu
from jax.sharding import PartitionSpec as P

HEAD_DIM = 128
TILE = 128
REACH = 2
CAP = 2
OFFSETS = (-2, 2, -1, 1)
AHEAD = 3
LOG2E = 1.4426950408889634
MESH = pl.DeviceIdType.MESH


def lowest_bit(bits):
    return bits & -bits


def kernel(
    query_hbm,
    key_hbm,
    value_hbm,
    select,
    counts,
    guide_scale,
    out_hbm,
    queries,
    own,
    staged,
    pool,
    branch_out,
    theirs,
    mixed,
    bias,
    send_bits,
    load_sem,
    send_sem,
    recv_sem,
    swap_send_sem,
    swap_recv_sem,
    out_sem,
):
    heads, tokens, _ = queries.shape
    tiles_dev = tokens // TILE
    half_rows = tokens // 2
    picks = select.shape[0]
    devices = lax.axis_size("seq")
    shards = devices // 2
    me = lax.axis_index("seq")
    shard = me // 2
    half = me % 2
    partner = me + 1 - 2 * half
    places = range(len(OFFSETS))

    def inside(place, sign):
        other = shard + sign * OFFSETS[place]
        return (other >= 0) & (other < shards)

    def columns(head):
        return pl.ds(pl.multiple_of(head * HEAD_DIM, HEAD_DIM), HEAD_DIM)

    def load(head, which):
        source = (key_hbm, value_hbm, query_hbm)[which]
        target = queries.at[head] if which == 2 else own.at[head, which]
        return pltpu.make_async_copy(
            source.at[:, columns(head)], target, load_sem.at[head, which]
        )

    def send(head, place):
        target = jnp.clip(me + 2 * OFFSETS[place], 0, devices - 1)
        return pltpu.make_async_remote_copy(
            src_ref=staged.at[head, place],
            dst_ref=pool.at[head, place],
            send_sem=send_sem.at[head, place],
            recv_sem=recv_sem.at[head, place],
            device_id={"seq": target},
            device_id_type=MESH,
        )

    def swap(head):
        return pltpu.make_async_remote_copy(
            src_ref=branch_out.at[head, pl.ds((1 - half) * half_rows, half_rows)],
            dst_ref=theirs.at[head],
            send_sem=swap_send_sem.at[head],
            recv_sem=swap_recv_sem.at[head],
            device_id={"seq": partner},
            device_id_type=MESH,
        )

    def write(head):
        return pltpu.make_async_copy(
            mixed.at[head], out_hbm.at[:, columns(head)], out_sem.at[head]
        )

    def start_loads(head, carry):
        for which in range(3):
            load(head, which).start()
        return carry

    lax.fori_loop(0, heads, start_loads, 0)

    barrier = pltpu.get_barrier_semaphore()
    pl.semaphore_signal(barrier, inc=1, device_id={"seq": partner}, device_id_type=MESH)
    greeted = jnp.int32(1)
    for place in places:
        there = inside(place, 1)
        greeted += there.astype(jnp.int32)

        @pl.when(there)
        def _():
            pl.semaphore_signal(
                barrier,
                inc=1,
                device_id={"seq": me + 2 * OFFSETS[place]},
                device_id_type=MESH,
            )

    for place in places:
        asker = jnp.clip(shard + OFFSETS[place], 0, shards - 1)
        bits = jnp.int32(0)
        for row in range(tiles_dev):
            live = counts[asker * tiles_dev + row]
            for pick in range(picks):
                tile = select[pick, asker * tiles_dev + row] - shard * tiles_dev
                wanted = (pick < live) & (tile >= 0) & (tile < tiles_dev)
                bits |= jnp.where(wanted, 1 << (tile & (tiles_dev - 1)), 0)
        first = lowest_bit(bits)
        send_bits[2 * place] = first
        send_bits[2 * place + 1] = lowest_bit(bits ^ first)

    first_tile = (shard - REACH) * tiles_dev
    row_bits = []
    for row in range(tiles_dev):
        live = counts[shard * tiles_dev + row]
        bits = jnp.int32(0)
        for pick in range(picks):
            tile = select[pick, shard * tiles_dev + row] - first_tile
            bits |= jnp.where(pick < live, 1 << (tile & 31), 0)
        row_bits.append(bits)
    union = row_bits[0]
    for bits in row_bits[1:]:
        union |= bits
    pool_bits = [1 << (REACH * tiles_dev + tile) for tile in range(tiles_dev)]
    for place in places:
        base = (REACH - OFFSETS[place]) * tiles_dev
        block = union & (((1 << tiles_dev) - 1) << base)
        first = lowest_bit(block)
        pool_bits += [first, lowest_bit(block ^ first)]
    pool_tiles = len(pool_bits)
    for row in range(tiles_dev):
        for slot, bit in enumerate(pool_bits):
            bias[row * pool_tiles + slot] = jnp.where(
                (row_bits[row] & bit) != 0, jnp.float32(0), jnp.float32(-jnp.inf)
            )

    for place in places:

        @pl.when(jnp.logical_not(inside(place, -1)))
        def _():
            def clear(head, carry):
                pool[head, place] = jnp.zeros(pool.shape[2:], pool.dtype)
                return carry

            lax.fori_loop(0, heads, clear, 0)

    def stage(head):
        for which in range(2):
            load(head, which).wait()
        for which in range(2):
            tiles = [own[head, which, tile * TILE : (tile + 1) * TILE] for tile in range(tiles_dev)]
            for place in places:
                for slot in range(CAP):
                    bit = send_bits[2 * place + slot]
                    chosen = tiles[-1]
                    for tile in range(tiles_dev - 1):
                        chosen = jnp.where(bit == 1 << tile, tiles[tile], chosen)
                    row = (which * CAP + slot) * TILE
                    staged[head, place, row : row + TILE] = chosen

    def start_sends(head):
        for place in places:

            @pl.when(inside(place, 1))
            def _():
                send(head, place).start()

    stage(0)
    pl.semaphore_wait(barrier, greeted)

    def fill(head, carry):
        stage(head)

        @pl.when(head <= AHEAD)
        def _():
            start_sends(head - 1)

        return carry

    lax.fori_loop(1, heads, fill, 0)

    factor = HEAD_DIM ** (-0.5) * LOG2E
    across = (((1,), (1,)), ((), ()))

    def attend(head, side):
        rows = pl.multiple_of(side * half_rows, half_rows)
        query = queries[head, pl.ds(rows, half_rows)]
        raw = [lax.dot_general(query, own[head, 0], across, preferred_element_type=jnp.float32)]
        for place in places:
            raw.append(
                lax.dot_general(
                    query,
                    pool[head, place, : CAP * TILE],
                    across,
                    preferred_element_type=jnp.float32,
                )
            )
        blocks = []
        for block in raw:
            blocks += [block[:, at : at + TILE] for at in range(0, block.shape[1], TILE)]
        parts = []
        for part in range(half_rows // TILE):
            row = side * (half_rows // TILE) + part
            scores = [
                block[part * TILE : (part + 1) * TILE] + bias[row * pool_tiles + slot]
                for slot, block in enumerate(blocks)
            ]
            peak = scores[0]
            for score in scores[1:]:
                peak = jnp.maximum(peak, score)
            peak = jnp.max(peak, axis=1, keepdims=True)
            weights = [jnp.exp2((score - peak) * factor) for score in scores]
            total = weights[0]
            for weight in weights[1:]:
                total = total + weight
            total = jnp.sum(total, axis=1, keepdims=True)
            weights = [weight.astype(jnp.bfloat16) for weight in weights]
            parts.append((weights, total))
        stacked = [
            jnp.concatenate([weights[slot] for weights, _ in parts], axis=0)
            for slot in range(pool_tiles)
        ]
        totals = jnp.concatenate([total for _, total in parts], axis=0)
        update = jnp.dot(
            jnp.concatenate(stacked[:tiles_dev], axis=1),
            own[head, 1],
            preferred_element_type=jnp.float32,
        )
        for place in places:
            at = tiles_dev + CAP * place
            update += jnp.dot(
                jnp.concatenate(stacked[at : at + CAP], axis=1),
                pool[head, place, CAP * TILE :],
                preferred_element_type=jnp.float32,
            )
        branch_out[head, pl.ds(rows, half_rows)] = (update / totals).astype(jnp.bfloat16)

    guidance = guide_scale[0]

    def combine(head):
        swap(head).wait_recv()
        rows = pl.multiple_of(half * half_rows, half_rows)
        mine = branch_out[head, pl.ds(rows, half_rows)].astype(jnp.float32)
        other = theirs[head].astype(jnp.float32)
        cond_out = jnp.where(half == 0, mine, other)
        uncond = jnp.where(half == 0, other, mine)
        mixed[head] = (uncond + guidance * (cond_out - uncond)).astype(jnp.bfloat16)
        write(head).start()

    def step(head, carry):
        load(head, 2).wait()
        for place in places:

            @pl.when(inside(place, -1))
            def _():
                send(head, place).wait_recv()

        @pl.when(head + AHEAD < heads)
        def _():
            start_sends(head + AHEAD)

        attend(head, 1 - half)
        attend(head, half)
        swap(head).start()

        @pl.when(head > 0)
        def _():
            combine(head - 1)

        return carry

    lax.fori_loop(0, heads, step, 0)
    combine(heads - 1)

    def finish(head, carry):
        for place in places:

            @pl.when(inside(place, 1))
            def _():
                send(head, place).wait_send()

        swap(head).wait_send()
        write(head).wait()
        return carry

    lax.fori_loop(0, heads, finish, 0)


def body(query_rows, key_rows, value_rows, select, counts, guide_scale):
    tokens, width = query_rows.shape
    heads = width // HEAD_DIM
    tiles_dev = tokens // TILE
    half_rows = tokens // 2
    places = len(OFFSETS)
    pool_tiles = tiles_dev + places * CAP
    kind = query_rows.dtype
    hbm = pl.BlockSpec(memory_space=pl.ANY)
    smem = pl.BlockSpec(memory_space=pltpu.SMEM)
    sent = (heads, places, 2 * CAP * TILE, HEAD_DIM)
    return pl.pallas_call(
        kernel,
        out_shape=jax.ShapeDtypeStruct((half_rows, width), kind),
        in_specs=[hbm, hbm, hbm, smem, smem, smem],
        out_specs=hbm,
        scratch_shapes=[
            pltpu.VMEM((heads, tokens, HEAD_DIM), kind),
            pltpu.VMEM((heads, 2, tokens, HEAD_DIM), kind),
            pltpu.VMEM(sent, kind),
            pltpu.VMEM(sent, kind),
            pltpu.VMEM((heads, tokens, HEAD_DIM), kind),
            pltpu.VMEM((heads, half_rows, HEAD_DIM), kind),
            pltpu.VMEM((heads, half_rows, HEAD_DIM), kind),
            pltpu.SMEM((tiles_dev * pool_tiles,), jnp.float32),
            pltpu.SMEM((places * CAP,), jnp.int32),
            pltpu.SemaphoreType.DMA((heads, 3)),
            pltpu.SemaphoreType.DMA((heads, places)),
            pltpu.SemaphoreType.DMA((heads, places)),
            pltpu.SemaphoreType.DMA((heads,)),
            pltpu.SemaphoreType.DMA((heads,)),
            pltpu.SemaphoreType.DMA((heads,)),
        ],
        compiler_params=pltpu.CompilerParams(
            collective_id=0, has_side_effects=True, vmem_limit_bytes=62 * 1024 * 1024
        ),
        name="sparse_attention",
    )(query_rows, key_rows, value_rows, select.T, counts, guide_scale)


def solution(mesh):
    rows = P(("groups", "seq"), None)
    in_specs = (rows, rows, rows, P("groups", None), P("groups"), P("groups"))
    return jax.shard_map(body, mesh=mesh, in_specs=in_specs, out_specs=rows, check_vma=False)
```

```python
import jax
import jax.numpy as jnp
from jax import lax
from jax.experimental import pallas as pl
from jax.experimental.pallas import tpu as pltpu
from jax.sharding import PartitionSpec as P

HEAD_DIM = 128
TILE = 128
REACH = 2
CAP = 2
OFFSETS = (-2, 2, -1, 1)
AHEAD = 3
LOG2E = 1.4426950408889634
MESH = pl.DeviceIdType.MESH


def lowest_bit(bits):
    return bits & -bits


def kernel(
    query_hbm,
    key_hbm,
    value_hbm,
    select_hbm,
    counts_hbm,
    guide_scale,
    out,
    queries,
    own,
    staged,
    pool,
    branch_out,
    theirs,
    select,
    counts,
    bias,
    send_bits,
    load_sem,
    send_sem,
    recv_sem,
    swap_send_sem,
    swap_recv_sem,
    table_sem,
):
    heads, tokens, _ = queries.shape
    tiles_dev = tokens // TILE
    half_rows = tokens // 2
    picks = select.shape[0]
    devices = lax.axis_size("seq")
    shards = devices // 2
    me = lax.axis_index("seq")
    shard = me // 2
    half = me % 2
    partner = me + 1 - 2 * half
    places = range(len(OFFSETS))

    def inside(place, sign):
        other = shard + sign * OFFSETS[place]
        return (other >= 0) & (other < shards)

    def columns(head):
        return pl.ds(pl.multiple_of(head * HEAD_DIM, HEAD_DIM), HEAD_DIM)

    def load(head, which):
        source = (key_hbm, value_hbm, query_hbm)[which]
        target = queries.at[head] if which == 2 else own.at[head, which]
        return pltpu.make_async_copy(
            source.at[:, columns(head)], target, load_sem.at[head, which]
        )

    def send(head, place):
        target = jnp.clip(me + 2 * OFFSETS[place], 0, devices - 1)
        return pltpu.make_async_remote_copy(
            src_ref=staged.at[head, place],
            dst_ref=pool.at[head, place],
            send_sem=send_sem.at[head, place],
            recv_sem=recv_sem.at[head, place],
            device_id={"seq": target},
            device_id_type=MESH,
        )

    def swap(head):
        return pltpu.make_async_remote_copy(
            src_ref=branch_out.at[head, pl.ds((1 - half) * half_rows, half_rows)],
            dst_ref=theirs.at[head],
            send_sem=swap_send_sem.at[head],
            recv_sem=swap_recv_sem.at[head],
            device_id={"seq": partner},
            device_id_type=MESH,
        )

    barrier = pltpu.get_barrier_semaphore()
    pl.semaphore_signal(barrier, inc=1, device_id={"seq": partner}, device_id_type=MESH)
    greeted = jnp.int32(1)
    for place in places:
        there = inside(place, 1)
        greeted += there.astype(jnp.int32)

        @pl.when(there)
        def _():
            pl.semaphore_signal(
                barrier,
                inc=1,
                device_id={"seq": me + 2 * OFFSETS[place]},
                device_id_type=MESH,
            )

    tables = [
        pltpu.make_async_copy(source, target, table_sem.at[at])
        for at, (source, target) in enumerate(((select_hbm, select), (counts_hbm, counts)))
    ]
    for table in tables:
        table.start()
    for which in range(2):
        load(0, which).start()

    def start_loads(head, carry):
        for which in range(2):
            load(head, which).start()
        return carry

    def start_query_loads(head, carry):
        load(head, 2).start()
        return carry

    lax.fori_loop(1, heads, start_loads, 0)
    lax.fori_loop(0, heads, start_query_loads, 0)
    for table in tables:
        table.wait()

    for place in places:
        asker = jnp.clip(shard + OFFSETS[place], 0, shards - 1)
        bits = jnp.int32(0)
        for row in range(tiles_dev):
            live = counts[asker * tiles_dev + row]
            for pick in range(picks):
                tile = select[pick, asker * tiles_dev + row] - shard * tiles_dev
                wanted = (pick < live) & (tile >= 0) & (tile < tiles_dev)
                bits |= jnp.where(wanted, 1 << (tile & (tiles_dev - 1)), 0)
        first = lowest_bit(bits)
        send_bits[2 * place] = first
        send_bits[2 * place + 1] = lowest_bit(bits ^ first)

    def stage(head):
        for which in range(2):
            load(head, which).wait()
        for which in range(2):
            tiles = [own[head, which, tile * TILE : (tile + 1) * TILE] for tile in range(tiles_dev)]
            for place in places:
                for slot in range(CAP):
                    bit = send_bits[2 * place + slot]
                    chosen = tiles[-1]
                    for tile in range(tiles_dev - 1):
                        chosen = jnp.where(bit == 1 << tile, tiles[tile], chosen)
                    row = (which * CAP + slot) * TILE
                    staged[head, place, row : row + TILE] = chosen

    def start_sends(head):
        for place in places:

            @pl.when(inside(place, 1))
            def _():
                send(head, place).start()

    stage(0)

    first_tile = (shard - REACH) * tiles_dev
    row_bits = []
    for row in range(tiles_dev):
        live = counts[shard * tiles_dev + row]
        bits = jnp.int32(0)
        for pick in range(picks):
            tile = select[pick, shard * tiles_dev + row] - first_tile
            bits |= jnp.where(pick < live, 1 << (tile & 31), 0)
        row_bits.append(bits)
    union = row_bits[0]
    for bits in row_bits[1:]:
        union |= bits
    pool_bits = [1 << (REACH * tiles_dev + tile) for tile in range(tiles_dev)]
    for place in places:
        base = (REACH - OFFSETS[place]) * tiles_dev
        block = union & (((1 << tiles_dev) - 1) << base)
        first = lowest_bit(block)
        pool_bits += [first, lowest_bit(block ^ first)]
    pool_tiles = len(pool_bits)
    for row in range(tiles_dev):
        for slot, bit in enumerate(pool_bits):
            bias[row * pool_tiles + slot] = jnp.where(
                (row_bits[row] & bit) != 0, jnp.float32(0), jnp.float32(-jnp.inf)
            )

    pl.semaphore_wait(barrier, greeted)
    start_sends(0)

    for place in places:

        @pl.when(jnp.logical_not(inside(place, -1)))
        def _():
            def clear(head, carry):
                pool[head, place] = jnp.zeros(pool.shape[2:], pool.dtype)
                return carry

            lax.fori_loop(0, heads, clear, 0)

    def fill(head, carry):
        stage(head)

        @pl.when(head < AHEAD)
        def _():
            start_sends(head)

        return carry

    lax.fori_loop(1, heads, fill, 0)

    factor = HEAD_DIM ** (-0.5) * LOG2E
    across = (((1,), (1,)), ((), ()))

    def attend(head, side):
        rows = pl.multiple_of(side * half_rows, half_rows)
        query = queries[head, pl.ds(rows, half_rows)]
        raw = [lax.dot_general(query, own[head, 0], across, preferred_element_type=jnp.float32)]
        for place in places:
            raw.append(
                lax.dot_general(
                    query,
                    pool[head, place, : CAP * TILE],
                    across,
                    preferred_element_type=jnp.float32,
                )
            )
        blocks = []
        for block in raw:
            blocks += [block[:, at : at + TILE] for at in range(0, block.shape[1], TILE)]
        parts = []
        for part in range(half_rows // TILE):
            row = side * (half_rows // TILE) + part
            scores = [
                block[part * TILE : (part + 1) * TILE] + bias[row * pool_tiles + slot]
                for slot, block in enumerate(blocks)
            ]
            peak = scores[0]
            for score in scores[1:]:
                peak = jnp.maximum(peak, score)
            peak = jnp.max(peak, axis=1, keepdims=True)
            weights = [jnp.exp2((score - peak) * factor) for score in scores]
            total = weights[0]
            for weight in weights[1:]:
                total = total + weight
            total = jnp.sum(total, axis=1, keepdims=True)
            weights = [weight.astype(jnp.bfloat16) for weight in weights]
            parts.append((weights, total))
        stacked = [
            jnp.concatenate([weights[slot] for weights, _ in parts], axis=0)
            for slot in range(pool_tiles)
        ]
        totals = jnp.concatenate([total for _, total in parts], axis=0)
        update = jnp.dot(
            jnp.concatenate(stacked[:tiles_dev], axis=1),
            own[head, 1],
            preferred_element_type=jnp.float32,
        )
        for place in places:
            at = tiles_dev + CAP * place
            update += jnp.dot(
                jnp.concatenate(stacked[at : at + CAP], axis=1),
                pool[head, place, CAP * TILE :],
                preferred_element_type=jnp.float32,
            )
        branch_out[head, pl.ds(rows, half_rows)] = (update / totals).astype(jnp.bfloat16)

    guidance = guide_scale[0]

    def combine(head):
        swap(head).wait_recv()
        rows = pl.multiple_of(half * half_rows, half_rows)
        mine = branch_out[head, pl.ds(rows, half_rows)].astype(jnp.float32)
        other = theirs[head].astype(jnp.float32)
        cond_out = jnp.where(half == 0, mine, other)
        uncond = jnp.where(half == 0, other, mine)
        mixed = uncond + guidance * (cond_out - uncond)
        out[:, columns(head)] = mixed.astype(out.dtype)

    def step(head, carry):
        load(head, 2).wait()
        for place in places:

            @pl.when(inside(place, -1))
            def _():
                send(head, place).wait_recv()

        @pl.when(head + AHEAD < heads)
        def _():
            start_sends(head + AHEAD)

        attend(head, 1 - half)
        swap(head).start()
        attend(head, half)

        @pl.when(head > 0)
        def _():
            combine(head - 1)

        return carry

    lax.fori_loop(0, heads, step, 0)
    combine(heads - 1)

    def finish(head, carry):
        for place in places:

            @pl.when(inside(place, 1))
            def _():
                send(head, place).wait_send()

        swap(head).wait_send()
        return carry

    lax.fori_loop(0, heads, finish, 0)


def body(query_rows, key_rows, value_rows, select, counts, guide_scale):
    tokens, width = query_rows.shape
    heads = width // HEAD_DIM
    tiles_dev = tokens // TILE
    half_rows = tokens // 2
    places = len(OFFSETS)
    pool_tiles = tiles_dev + places * CAP
    kind = query_rows.dtype
    hbm = pl.BlockSpec(memory_space=pltpu.HBM)
    sent = (heads, places, 2 * CAP * TILE, HEAD_DIM)
    operands = [
        pltpu.with_memory_space_constraint(operand, pltpu.HBM)
        for operand in (query_rows, key_rows, value_rows, select.T, counts)
    ]
    return pl.pallas_call(
        kernel,
        out_shape=pltpu.VMEM((half_rows, width), kind),
        in_specs=[hbm] * 5 + [pl.BlockSpec(memory_space=pltpu.SMEM)],
        out_specs=pl.BlockSpec(memory_space=pltpu.VMEM),
        scratch_shapes=[
            pltpu.VMEM((heads, tokens, HEAD_DIM), kind),
            pltpu.VMEM((heads, 2, tokens, HEAD_DIM), kind),
            pltpu.VMEM(sent, kind),
            pltpu.VMEM(sent, kind),
            pltpu.VMEM((heads, tokens, HEAD_DIM), kind),
            pltpu.VMEM((heads, half_rows, HEAD_DIM), kind),
            pltpu.SMEM(select.shape[::-1], select.dtype),
            pltpu.SMEM(counts.shape, counts.dtype),
            pltpu.SMEM((tiles_dev * pool_tiles,), jnp.float32),
            pltpu.SMEM((places * CAP,), jnp.int32),
            pltpu.SemaphoreType.DMA((heads, 3)),
            pltpu.SemaphoreType.DMA((heads, places)),
            pltpu.SemaphoreType.DMA((heads, places)),
            pltpu.SemaphoreType.DMA((heads,)),
            pltpu.SemaphoreType.DMA((heads,)),
            pltpu.SemaphoreType.DMA((2,)),
        ],
        compiler_params=pltpu.CompilerParams(
            collective_id=0, has_side_effects=True, vmem_limit_bytes=48 * 1024 * 1024
        ),
        name="sparse_attention",
    )(*operands, guide_scale)


def solution(mesh):
    rows = P(("groups", "seq"), None)
    in_specs = (rows, rows, rows, P("groups", None), P("groups"), P("groups"))
    return jax.shard_map(body, mesh=mesh, in_specs=in_specs, out_specs=rows, check_vma=False)
```

```python
import functools

import jax
import jax.numpy as jnp
from jax import lax
from jax.experimental import pallas as pl
from jax.experimental.pallas import tpu as pltpu
from jax.sharding import PartitionSpec as P

HEAD_DIM = 128
TILE = 128
REACH = 2
CAP = 2
OFFSETS = (-2, 2, -1, 1)
LAG = 2
LOG2E = 1.4426950408889634
MESH = pl.DeviceIdType.MESH


def lowest_bit(bits):
    return bits & -bits


def kernel(
    row_shards,
    query_hbm,
    key_hbm,
    value_hbm,
    select_hbm,
    counts_hbm,
    guide_scale,
    out,
    queries,
    own,
    staged,
    pool,
    branch_out,
    theirs,
    select,
    counts,
    bias,
    send_bits,
    load_sem,
    send_sem,
    recv_sem,
    swap_send_sem,
    swap_recv_sem,
    table_sem,
    ready,
):
    heads, tokens, _ = queries.shape
    tiles_dev = tokens // TILE
    half_rows = tokens // 2
    picks = select.shape[0]
    devices = lax.axis_size("seq")
    shards = devices // 2
    me = lax.axis_index("seq")
    shard = me // 2
    half = me % 2
    partner = me + 1 - 2 * half
    places = range(len(OFFSETS))
    spot = shard % row_shards

    def inside(place, sign):
        other = shard + sign * OFFSETS[place]
        return (other >= 0) & (other < shards)

    def crosses(place):
        ahead = spot + OFFSETS[place]
        return ahead >= row_shards if OFFSETS[place] > 0 else ahead < 0

    def earlier(place):
        return crosses(place) if OFFSETS[place] > 0 else jnp.logical_not(crosses(place))

    def columns(head):
        return pl.ds(pl.multiple_of(head * HEAD_DIM, HEAD_DIM), HEAD_DIM)

    def load(head, which):
        source = (key_hbm, value_hbm, query_hbm)[which]
        target = queries.at[head] if which == 2 else own.at[head, which]
        return pltpu.make_async_copy(
            source.at[:, columns(head)], target, load_sem.at[head, which]
        )

    def send(head, place):
        target = jnp.clip(me + 2 * OFFSETS[place], 0, devices - 1)
        return pltpu.make_async_remote_copy(
            src_ref=staged.at[head, place],
            dst_ref=pool.at[head, place],
            send_sem=send_sem.at[head, place],
            recv_sem=recv_sem.at[head, place],
            device_id={"seq": target},
            device_id_type=MESH,
        )

    def swap(head):
        return pltpu.make_async_remote_copy(
            src_ref=branch_out.at[head, pl.ds((1 - half) * half_rows, half_rows)],
            dst_ref=theirs.at[head],
            send_sem=swap_send_sem.at[head],
            recv_sem=swap_recv_sem.at[head],
            device_id={"seq": partner},
            device_id_type=MESH,
        )

    barrier = pltpu.get_barrier_semaphore()

    def greet(shift):
        pl.semaphore_signal(barrier, inc=1, device_id={"seq": me + shift}, device_id_type=MESH)

    greet(1 - 2 * half)
    awaited = jnp.int32(1)
    for place in places:
        there = inside(place, 1)
        awaited += (there & earlier(place)).astype(jnp.int32)

        @pl.when(there & jnp.logical_not(earlier(place)))
        def _():
            greet(2 * OFFSETS[place])

    tables = [
        pltpu.make_async_copy(source, target, table_sem.at[at])
        for at, (source, target) in enumerate(((select_hbm, select), (counts_hbm, counts)))
    ]
    for table in tables:
        table.start()
    for which in range(2):
        load(0, which).start()

    def start_loads(head, carry):
        for which in range(2):
            load(head, which).start()
        return carry

    def start_query_loads(head, carry):
        load(head, 2).start()
        return carry

    lax.fori_loop(1, heads, start_loads, 0)
    lax.fori_loop(0, heads, start_query_loads, 0)
    for table in tables:
        table.wait()

    for place in places:
        asker = jnp.clip(shard + OFFSETS[place], 0, shards - 1)
        bits = jnp.int32(0)
        for row in range(tiles_dev):
            live = counts[asker * tiles_dev + row]
            for pick in range(picks):
                tile = select[pick, asker * tiles_dev + row] - shard * tiles_dev
                wanted = (pick < live) & (tile >= 0) & (tile < tiles_dev)
                bits |= jnp.where(wanted, 1 << (tile & (tiles_dev - 1)), 0)
        first = lowest_bit(bits)
        send_bits[2 * place] = first
        send_bits[2 * place + 1] = lowest_bit(bits ^ first)

    def stage(head):
        for which in range(2):
            load(head, which).wait()
        for which in range(2):
            tiles = [own[head, which, tile * TILE : (tile + 1) * TILE] for tile in range(tiles_dev)]
            for place in places:
                for slot in range(CAP):
                    bit = send_bits[2 * place + slot]
                    chosen = tiles[-1]
                    for tile in range(tiles_dev - 1):
                        chosen = jnp.where(bit == 1 << tile, tiles[tile], chosen)
                    row = (which * CAP + slot) * TILE
                    staged[head, place, row : row + TILE] = chosen

    def start_early(head):
        for place in places:
            there = inside(place, 1) & earlier(place)
            behind = crosses(place) if OFFSETS[place] == REACH else jnp.bool_(False)
            at = jnp.where(behind & (spot == row_shards - 1), head - LAG, head)

            @pl.when(there & (at >= 0) & (at < heads))
            def _():
                send(at, place).start()

    stage(0)

    pl.semaphore_wait(barrier, awaited)
    for place in places:

        @pl.when(inside(place, 1) & earlier(place))
        def _():
            pl.semaphore_signal(
                ready.at[OFFSETS.index(-OFFSETS[place])],
                inc=1,
                device_id={"seq": me + 2 * OFFSETS[place]},
                device_id_type=MESH,
            )

    start_early(0)

    first_tile = (shard - REACH) * tiles_dev
    row_bits = []
    for row in range(tiles_dev):
        live = counts[shard * tiles_dev + row]
        bits = jnp.int32(0)
        for pick in range(picks):
            tile = select[pick, shard * tiles_dev + row] - first_tile
            bits |= jnp.where(pick < live, 1 << (tile & 31), 0)
        row_bits.append(bits)
    union = row_bits[0]
    for bits in row_bits[1:]:
        union |= bits
    pool_bits = [1 << (REACH * tiles_dev + tile) for tile in range(tiles_dev)]
    for place in places:
        base = (REACH - OFFSETS[place]) * tiles_dev
        block = union & (((1 << tiles_dev) - 1) << base)
        first = lowest_bit(block)
        pool_bits += [first, lowest_bit(block ^ first)]
    pool_tiles = len(pool_bits)
    for row in range(tiles_dev):
        for slot, bit in enumerate(pool_bits):
            bias[row * pool_tiles + slot] = jnp.where(
                (row_bits[row] & bit) != 0, jnp.float32(0), jnp.float32(-jnp.inf)
            )


    for place in places:

        @pl.when(jnp.logical_not(inside(place, -1)))
        def _():
            def clear(head, carry):
                pool[head, place] = jnp.zeros(pool.shape[2:], pool.dtype)
                return carry

            lax.fori_loop(0, heads, clear, 0)

    def fill(head, carry):
        stage(head)
        start_early(head)
        return carry

    lax.fori_loop(1, heads, fill, 0)
    for extra in range(LAG):
        start_early(heads + extra)

    for ahead in (True, False):
        some = [place for place in places if (OFFSETS[place] > 0) == ahead]
        later = [inside(place, 1) & jnp.logical_not(earlier(place)) for place in some]
        for place, there in zip(some, later):

            @pl.when(there)
            def _():
                pl.semaphore_wait(ready.at[place], 1)

        def start_later(head, carry):
            for place, there in zip(some, later):

                @pl.when(there)
                def _():
                    send(head, place).start()

            return carry

        lax.fori_loop(0, heads, start_later, 0)

    factor = HEAD_DIM ** (-0.5) * LOG2E
    across = (((1,), (1,)), ((), ()))

    def attend(head, side):
        rows = pl.multiple_of(side * half_rows, half_rows)
        query = queries[head, pl.ds(rows, half_rows)]
        raw = [lax.dot_general(query, own[head, 0], across, preferred_element_type=jnp.float32)]
        for place in places:
            raw.append(
                lax.dot_general(
                    query,
                    pool[head, place, : CAP * TILE],
                    across,
                    preferred_element_type=jnp.float32,
                )
            )
        blocks = []
        for block in raw:
            blocks += [block[:, at : at + TILE] for at in range(0, block.shape[1], TILE)]
        parts = []
        for part in range(half_rows // TILE):
            row = side * (half_rows // TILE) + part
            scores = [
                block[part * TILE : (part + 1) * TILE] + bias[row * pool_tiles + slot]
                for slot, block in enumerate(blocks)
            ]
            peak = scores[0]
            for score in scores[1:]:
                peak = jnp.maximum(peak, score)
            peak = jnp.max(peak, axis=1, keepdims=True)
            weights = [jnp.exp2((score - peak) * factor) for score in scores]
            total = weights[0]
            for weight in weights[1:]:
                total = total + weight
            total = jnp.sum(total, axis=1, keepdims=True)
            weights = [weight.astype(jnp.bfloat16) for weight in weights]
            parts.append((weights, total))
        stacked = [
            jnp.concatenate([weights[slot] for weights, _ in parts], axis=0)
            for slot in range(pool_tiles)
        ]
        totals = jnp.concatenate([total for _, total in parts], axis=0)
        update = jnp.dot(
            jnp.concatenate(stacked[:tiles_dev], axis=1),
            own[head, 1],
            preferred_element_type=jnp.float32,
        )
        for place in places:
            at = tiles_dev + CAP * place
            update += jnp.dot(
                jnp.concatenate(stacked[at : at + CAP], axis=1),
                pool[head, place, CAP * TILE :],
                preferred_element_type=jnp.float32,
            )
        branch_out[head, pl.ds(rows, half_rows)] = (update / totals).astype(jnp.bfloat16)

    guidance = guide_scale[0]

    def combine(head):
        swap(head).wait_recv()
        rows = pl.multiple_of(half * half_rows, half_rows)
        mine = branch_out[head, pl.ds(rows, half_rows)].astype(jnp.float32)
        other = theirs[head].astype(jnp.float32)
        cond_out = jnp.where(half == 0, mine, other)
        uncond = jnp.where(half == 0, other, mine)
        mixed = uncond + guidance * (cond_out - uncond)
        out[:, columns(head)] = mixed.astype(out.dtype)

    def step(head, carry):
        load(head, 2).wait()
        for place in places:

            @pl.when(inside(place, -1))
            def _():
                send(head, place).wait_recv()

        attend(head, 1 - half)
        swap(head).start()
        attend(head, half)

        @pl.when(head > 0)
        def _():
            combine(head - 1)

        return carry

    lax.fori_loop(0, heads, step, 0)

    def finish(head, carry):
        for place in places:

            @pl.when(inside(place, 1))
            def _():
                send(head, place).wait_send()

        return carry

    lax.fori_loop(0, heads, finish, 0)
    combine(heads - 1)

    def finish_swap(head, carry):
        swap(head).wait_send()
        return carry

    lax.fori_loop(0, heads, finish_swap, 0)


def body(row_shards, query_rows, key_rows, value_rows, select, counts, guide_scale):
    tokens, width = query_rows.shape
    heads = width // HEAD_DIM
    tiles_dev = tokens // TILE
    half_rows = tokens // 2
    places = len(OFFSETS)
    pool_tiles = tiles_dev + places * CAP
    kind = query_rows.dtype
    hbm = pl.BlockSpec(memory_space=pltpu.HBM)
    sent = (heads, places, 2 * CAP * TILE, HEAD_DIM)
    operands = [
        pltpu.with_memory_space_constraint(operand, pltpu.HBM)
        for operand in (query_rows, key_rows, value_rows, select.T, counts)
    ]
    return pl.pallas_call(
        functools.partial(kernel, row_shards),
        out_shape=pltpu.VMEM((half_rows, width), kind),
        in_specs=[hbm] * 5 + [pl.BlockSpec(memory_space=pltpu.SMEM)],
        out_specs=pl.BlockSpec(memory_space=pltpu.VMEM),
        scratch_shapes=[
            pltpu.VMEM((heads, tokens, HEAD_DIM), kind),
            pltpu.VMEM((heads, 2, tokens, HEAD_DIM), kind),
            pltpu.VMEM(sent, kind),
            pltpu.VMEM(sent, kind),
            pltpu.VMEM((heads, tokens, HEAD_DIM), kind),
            pltpu.VMEM((heads, half_rows, HEAD_DIM), kind),
            pltpu.SMEM(select.shape[::-1], select.dtype),
            pltpu.SMEM(counts.shape, counts.dtype),
            pltpu.SMEM((tiles_dev * pool_tiles,), jnp.float32),
            pltpu.SMEM((places * CAP,), jnp.int32),
            pltpu.SemaphoreType.DMA((heads, 3)),
            pltpu.SemaphoreType.DMA((heads, places)),
            pltpu.SemaphoreType.DMA((heads, places)),
            pltpu.SemaphoreType.DMA((heads,)),
            pltpu.SemaphoreType.DMA((heads,)),
            pltpu.SemaphoreType.DMA((2,)),
            pltpu.SemaphoreType.REGULAR((places,)),
        ],
        compiler_params=pltpu.CompilerParams(
            collective_id=0, has_side_effects=True, vmem_limit_bytes=48 * 1024 * 1024
        ),
        name="sparse_attention",
    )(*operands, guide_scale)


def solution(mesh):
    rows = P(("groups", "seq"), None)
    row_shards = len({device.coords[1] for device in mesh.devices.flat})
    local = functools.partial(body, row_shards)
    in_specs = (rows, rows, rows, P("groups", None), P("groups"), P("groups"))
    return jax.shard_map(local, mesh=mesh, in_specs=in_specs, out_specs=rows, check_vma=False)
```

```python
import functools

import jax
import jax.numpy as jnp
from jax import lax
from jax.experimental import pallas as pl
from jax.experimental.pallas import tpu as pltpu
from jax.sharding import PartitionSpec as P

HEAD_DIM = 128
TILE = 128
REACH = 2
CAP = 2
OFFSETS = (-2, -1, 2, 1)
LAG = 1
LOG2E = 1.4426950408889634
MESH = pl.DeviceIdType.MESH


def lowest_bit(bits):
    return bits & -bits


def kernel(
    row_shards,
    query_hbm,
    key_hbm,
    value_hbm,
    select_hbm,
    counts_hbm,
    guide_scale,
    out,
    queries,
    own,
    staged,
    pool,
    branch_out,
    theirs,
    select,
    counts,
    bias,
    send_bits,
    load_sem,
    send_sem,
    recv_sem,
    swap_send_sem,
    swap_recv_sem,
    table_sem,
    ready,
):
    heads, tokens, _ = queries.shape
    tiles_dev = tokens // TILE
    half_rows = tokens // 2
    picks = select.shape[0]
    devices = lax.axis_size("seq")
    shards = devices // 2
    me = lax.axis_index("seq")
    shard = me // 2
    half = me % 2
    partner = me + 1 - 2 * half
    places = range(len(OFFSETS))
    spot = shard % row_shards

    def inside(place, sign):
        other = shard + sign * OFFSETS[place]
        return (other >= 0) & (other < shards)

    def crosses(place):
        ahead = spot + OFFSETS[place]
        return ahead >= row_shards if OFFSETS[place] > 0 else ahead < 0

    def earlier(place):
        return crosses(place) if OFFSETS[place] > 0 else jnp.logical_not(crosses(place))

    def columns(head):
        return pl.ds(pl.multiple_of(head * HEAD_DIM, HEAD_DIM), HEAD_DIM)

    def load(head, which):
        source = (key_hbm, value_hbm, query_hbm)[which]
        target = queries.at[head] if which == 2 else own.at[head, which]
        return pltpu.make_async_copy(
            source.at[:, columns(head)], target, load_sem.at[head, which]
        )

    def send(head, place):
        target = jnp.clip(me + 2 * OFFSETS[place], 0, devices - 1)
        return pltpu.make_async_remote_copy(
            src_ref=staged.at[head, place],
            dst_ref=pool.at[head, place],
            send_sem=send_sem.at[head, place],
            recv_sem=recv_sem.at[head, place],
            device_id={"seq": target},
            device_id_type=MESH,
        )

    def swap(head):
        return pltpu.make_async_remote_copy(
            src_ref=branch_out.at[head, pl.ds((1 - half) * half_rows, half_rows)],
            dst_ref=theirs.at[head],
            send_sem=swap_send_sem.at[head],
            recv_sem=swap_recv_sem.at[head],
            device_id={"seq": partner},
            device_id_type=MESH,
        )

    tables = [
        pltpu.make_async_copy(source, target, table_sem.at[at])
        for at, (source, target) in enumerate(((select_hbm, select), (counts_hbm, counts)))
    ]
    for table in tables:
        table.start()
    for which in range(2):
        load(0, which).start()

    barrier = pltpu.get_barrier_semaphore()

    def greet(shift):
        pl.semaphore_signal(barrier, inc=1, device_id={"seq": me + shift}, device_id_type=MESH)

    greet(1 - 2 * half)
    awaited = jnp.int32(1)
    for place in places:
        there = inside(place, 1)
        awaited += (there & earlier(place)).astype(jnp.int32)

        @pl.when(there & jnp.logical_not(earlier(place)))
        def _():
            greet(2 * OFFSETS[place])

    def start_loads(head, carry):
        for which in range(2):
            load(head, which).start()
        return carry

    def start_query_loads(head, carry):
        load(head, 2).start()
        return carry

    lax.fori_loop(1, heads, start_loads, 0)
    lax.fori_loop(0, heads, start_query_loads, 0)
    pl.semaphore_wait(barrier, awaited)
    for place in places:

        @pl.when(inside(place, 1) & earlier(place))
        def _():
            pl.semaphore_signal(
                ready.at[OFFSETS.index(-OFFSETS[place])],
                inc=1,
                device_id={"seq": me + 2 * OFFSETS[place]},
                device_id_type=MESH,
            )

    for table in tables:
        table.wait()

    def find_wanted(place):
        asker = jnp.clip(shard + OFFSETS[place], 0, shards - 1)
        bits = jnp.int32(0)
        for row in range(tiles_dev):
            live = counts[asker * tiles_dev + row]
            for pick in range(picks):
                tile = select[pick, asker * tiles_dev + row]
                wanted = (pick < live) & (tile // tiles_dev == shard)
                bits |= jnp.where(wanted, 1 << tile % tiles_dev, 0)
        first = lowest_bit(bits)
        send_bits[2 * place] = first
        send_bits[2 * place + 1] = lowest_bit(bits ^ first)

    def stage(head, some):
        for which in range(2):
            tiles = [own[head, which, tile * TILE : (tile + 1) * TILE] for tile in range(tiles_dev)]
            for place in some:
                for slot in range(CAP):
                    bit = send_bits[2 * place + slot]
                    chosen = tiles[-1]
                    for tile in range(tiles_dev - 1):
                        chosen = jnp.where(bit == 1 << tile, tiles[tile], chosen)
                    row = (which * CAP + slot) * TILE
                    staged[head, place, row : row + TILE] = chosen

    def await_tiles(head):
        for which in range(2):
            load(head, which).wait()

    def start_early(head, some=places):
        for place in some:
            there = inside(place, 1) & earlier(place)
            behind = crosses(place) if OFFSETS[place] == REACH else jnp.bool_(False)
            at = jnp.where(behind & (spot == row_shards - 1), head - LAG, head)

            @pl.when(there & (at >= 0) & (at < heads))
            def _():
                send(at, place).start()

    for place in reversed(places):
        find_wanted(place)
        if place == len(OFFSETS) - 1:
            await_tiles(0)
        stage(0, [place])
        start_early(0, [place])

    first_tile = (shard - REACH) * tiles_dev
    row_bits = []
    for row in range(tiles_dev):
        live = counts[shard * tiles_dev + row]
        bits = jnp.int32(0)
        for pick in range(picks):
            tile = select[pick, shard * tiles_dev + row] - first_tile
            bits |= jnp.where(pick < live, 1 << (tile & 31), 0)
        row_bits.append(bits)
    union = row_bits[0]
    for bits in row_bits[1:]:
        union |= bits
    pool_bits = [1 << (REACH * tiles_dev + tile) for tile in range(tiles_dev)]
    for place in places:
        base = (REACH - OFFSETS[place]) * tiles_dev
        block = union & (((1 << tiles_dev) - 1) << base)
        first = lowest_bit(block)
        pool_bits += [first, lowest_bit(block ^ first)]
    pool_tiles = len(pool_bits)
    for row in range(tiles_dev):
        for slot, bit in enumerate(pool_bits):
            bias[row * pool_tiles + slot] = jnp.where(
                (row_bits[row] & bit) != 0, jnp.float32(0), jnp.float32(-jnp.inf)
            )


    for place in places:

        @pl.when(jnp.logical_not(inside(place, -1)))
        def _():
            def clear(head, carry):
                pool[head, place] = jnp.zeros(pool.shape[2:], pool.dtype)
                return carry

            lax.fori_loop(0, heads, clear, 0)

    def fill(head, carry):
        await_tiles(head)
        stage(head, places)
        start_early(head)
        return carry

    lax.fori_loop(1, heads, fill, 0)
    for extra in range(LAG):
        start_early(heads + extra)

    for ahead in (True, False):
        some = [place for place in places if (OFFSETS[place] > 0) == ahead]
        later = [inside(place, 1) & jnp.logical_not(earlier(place)) for place in some]
        for place, there in zip(some, later):

            @pl.when(there)
            def _():
                pl.semaphore_wait(ready.at[place], 1)

        def start_later(head, carry):
            for place, there in zip(some, later):

                @pl.when(there)
                def _():
                    send(head, place).start()

            return carry

        lax.fori_loop(0, heads, start_later, 0)

    factor = HEAD_DIM ** (-0.5) * LOG2E
    across = (((1,), (1,)), ((), ()))

    def attend(head, side):
        rows = pl.multiple_of(side * half_rows, half_rows)
        query = queries[head, pl.ds(rows, half_rows)]
        raw = [lax.dot_general(query, own[head, 0], across, preferred_element_type=jnp.float32)]
        for place in places:
            raw.append(
                lax.dot_general(
                    query,
                    pool[head, place, : CAP * TILE],
                    across,
                    preferred_element_type=jnp.float32,
                )
            )
        blocks = []
        for block in raw:
            blocks += [block[:, at : at + TILE] for at in range(0, block.shape[1], TILE)]
        parts = []
        for part in range(half_rows // TILE):
            row = side * (half_rows // TILE) + part
            scores = [
                block[part * TILE : (part + 1) * TILE] + bias[row * pool_tiles + slot]
                for slot, block in enumerate(blocks)
            ]
            peak = scores[0]
            for score in scores[1:]:
                peak = jnp.maximum(peak, score)
            peak = jnp.max(peak, axis=1, keepdims=True)
            weights = [jnp.exp2((score - peak) * factor) for score in scores]
            total = weights[0]
            for weight in weights[1:]:
                total = total + weight
            total = jnp.sum(total, axis=1, keepdims=True)
            weights = [weight.astype(jnp.bfloat16) for weight in weights]
            parts.append((weights, total))
        stacked = [
            jnp.concatenate([weights[slot] for weights, _ in parts], axis=0)
            for slot in range(pool_tiles)
        ]
        totals = jnp.concatenate([total for _, total in parts], axis=0)
        update = jnp.dot(
            jnp.concatenate(stacked[:tiles_dev], axis=1),
            own[head, 1],
            preferred_element_type=jnp.float32,
        )
        for place in places:
            at = tiles_dev + CAP * place
            update += jnp.dot(
                jnp.concatenate(stacked[at : at + CAP], axis=1),
                pool[head, place, CAP * TILE :],
                preferred_element_type=jnp.float32,
            )
        branch_out[head, pl.ds(rows, half_rows)] = (update / totals).astype(jnp.bfloat16)

    guidance = guide_scale[0]

    def combine(head):
        swap(head).wait_recv()
        rows = pl.multiple_of(half * half_rows, half_rows)
        mine = branch_out[head, pl.ds(rows, half_rows)].astype(jnp.float32)
        other = theirs[head].astype(jnp.float32)
        cond_out = jnp.where(half == 0, mine, other)
        uncond = jnp.where(half == 0, other, mine)
        mixed = uncond + guidance * (cond_out - uncond)
        out[:, columns(head)] = mixed.astype(out.dtype)

    def step(head, carry):
        load(head, 2).wait()
        for place in places:

            @pl.when(inside(place, -1))
            def _():
                send(head, place).wait_recv()

        attend(head, 1 - half)
        swap(head).start()
        attend(head, half)

        @pl.when(head > 0)
        def _():
            combine(head - 1)

        return carry

    lax.fori_loop(0, heads, step, 0)

    def finish(head, carry):
        for place in places:

            @pl.when(inside(place, 1))
            def _():
                send(head, place).wait_send()

        return carry

    lax.fori_loop(0, heads, finish, 0)
    combine(heads - 1)

    def finish_swap(head, carry):
        swap(head).wait_send()
        return carry

    lax.fori_loop(0, heads, finish_swap, 0)


def body(row_shards, query_rows, key_rows, value_rows, select, counts, guide_scale):
    tokens, width = query_rows.shape
    heads = width // HEAD_DIM
    tiles_dev = tokens // TILE
    half_rows = tokens // 2
    places = len(OFFSETS)
    pool_tiles = tiles_dev + places * CAP
    kind = query_rows.dtype
    hbm = pl.BlockSpec(memory_space=pltpu.HBM)
    sent = (heads, places, 2 * CAP * TILE, HEAD_DIM)
    operands = [
        pltpu.with_memory_space_constraint(operand, pltpu.HBM)
        for operand in (query_rows, key_rows, value_rows, select.T, counts)
    ]
    return pl.pallas_call(
        functools.partial(kernel, row_shards),
        out_shape=pltpu.VMEM((half_rows, width), kind),
        in_specs=[hbm] * 5 + [pl.BlockSpec(memory_space=pltpu.SMEM)],
        out_specs=pl.BlockSpec(memory_space=pltpu.VMEM),
        scratch_shapes=[
            pltpu.VMEM((heads, tokens, HEAD_DIM), kind),
            pltpu.VMEM((heads, 2, tokens, HEAD_DIM), kind),
            pltpu.VMEM(sent, kind),
            pltpu.VMEM(sent, kind),
            pltpu.VMEM((heads, tokens, HEAD_DIM), kind),
            pltpu.VMEM((heads, half_rows, HEAD_DIM), kind),
            pltpu.SMEM(select.shape[::-1], select.dtype),
            pltpu.SMEM(counts.shape, counts.dtype),
            pltpu.SMEM((tiles_dev * pool_tiles,), jnp.float32),
            pltpu.SMEM((places * CAP,), jnp.int32),
            pltpu.SemaphoreType.DMA((heads, 3)),
            pltpu.SemaphoreType.DMA((heads, places)),
            pltpu.SemaphoreType.DMA((heads, places)),
            pltpu.SemaphoreType.DMA((heads,)),
            pltpu.SemaphoreType.DMA((heads,)),
            pltpu.SemaphoreType.DMA((2,)),
            pltpu.SemaphoreType.REGULAR((places,)),
        ],
        compiler_params=pltpu.CompilerParams(
            collective_id=0, has_side_effects=True, vmem_limit_bytes=48 * 1024 * 1024
        ),
        name="sparse_attention",
    )(*operands, guide_scale)


def solution(mesh):
    rows = P(("groups", "seq"), None)
    row_shards = len({device.coords[1] for device in mesh.devices.flat})
    local = functools.partial(body, row_shards)
    in_specs = (rows, rows, rows, P("groups", None), P("groups"), P("groups"))
    return jax.shard_map(local, mesh=mesh, in_specs=in_specs, out_specs=rows, check_vma=False)
```

```python
import functools

import jax
import jax.numpy as jnp
from jax import lax
from jax.experimental import pallas as pl
from jax.experimental.pallas import tpu as pltpu
from jax.sharding import PartitionSpec as P

HEAD_DIM = 128
TILE = 128
REACH = 2
CAP = 2
OFFSETS = (-2, -1, 2, 1)
LAG = 1
LOG2E = 1.4426950408889634
MESH = pl.DeviceIdType.MESH


def lowest_bit(bits):
    return bits & -bits


def kernel(
    row_shards,
    query_hbm,
    key_hbm,
    value_hbm,
    select_hbm,
    counts_hbm,
    guide_scale,
    out,
    queries,
    own,
    staged,
    pool,
    branch_out,
    theirs,
    select,
    counts,
    bias,
    send_bits,
    load_sem,
    send_sem,
    recv_sem,
    swap_send_sem,
    swap_recv_sem,
    table_sem,
    ready,
):
    heads, tokens, _ = queries.shape
    tiles_dev = tokens // TILE
    half_rows = tokens // 2
    picks = select.shape[0]
    devices = lax.axis_size("seq")
    shards = devices // 2
    me = lax.axis_index("seq")
    shard = me // 2
    half = me % 2
    partner = me + 1 - 2 * half
    places = range(len(OFFSETS))
    spot = shard % row_shards

    def inside(place, sign):
        other = shard + sign * OFFSETS[place]
        return (other >= 0) & (other < shards)

    def crosses(place):
        ahead = spot + OFFSETS[place]
        return ahead >= row_shards if OFFSETS[place] > 0 else ahead < 0

    def earlier(place):
        return crosses(place) if OFFSETS[place] > 0 else jnp.logical_not(crosses(place))

    def columns(head):
        return pl.ds(pl.multiple_of(head * HEAD_DIM, HEAD_DIM), HEAD_DIM)

    def load(head, which):
        source = (key_hbm, value_hbm, query_hbm)[which]
        target = queries.at[head] if which == 2 else own.at[head, which]
        return pltpu.make_async_copy(
            source.at[:, columns(head)], target, load_sem.at[head, which]
        )

    def send(head, place):
        target = jnp.clip(me + 2 * OFFSETS[place], 0, devices - 1)
        return pltpu.make_async_remote_copy(
            src_ref=staged.at[head, place],
            dst_ref=pool.at[head, place],
            send_sem=send_sem.at[head, place],
            recv_sem=recv_sem.at[head, place],
            device_id={"seq": target},
            device_id_type=MESH,
        )

    def swap(head):
        return pltpu.make_async_remote_copy(
            src_ref=branch_out.at[head, pl.ds((1 - half) * half_rows, half_rows)],
            dst_ref=theirs.at[head],
            send_sem=swap_send_sem.at[head],
            recv_sem=swap_recv_sem.at[head],
            device_id={"seq": partner},
            device_id_type=MESH,
        )

    tables = [
        pltpu.make_async_copy(source, target, table_sem.at[at])
        for at, (source, target) in enumerate(((select_hbm, select), (counts_hbm, counts)))
    ]
    for table in tables:
        table.start()
    for which in range(2):
        load(0, which).start()

    barrier = pltpu.get_barrier_semaphore()

    def greet(shift):
        pl.semaphore_signal(barrier, inc=1, device_id={"seq": me + shift}, device_id_type=MESH)

    greet(1 - 2 * half)
    awaited = jnp.int32(1)
    for place in places:
        there = inside(place, 1)
        awaited += (there & earlier(place)).astype(jnp.int32)

        @pl.when(there & jnp.logical_not(earlier(place)))
        def _():
            greet(2 * OFFSETS[place])

    def start_loads(head, carry):
        for which in range(2):
            load(head, which).start()
        return carry

    def start_query_loads(head, carry):
        load(head, 2).start()
        return carry

    lax.fori_loop(1, heads, start_loads, 0)
    lax.fori_loop(0, heads, start_query_loads, 0)
    pl.semaphore_wait(barrier, awaited)
    for place in places:

        @pl.when(inside(place, 1) & earlier(place))
        def _():
            pl.semaphore_signal(
                ready.at[OFFSETS.index(-OFFSETS[place])],
                inc=1,
                device_id={"seq": me + 2 * OFFSETS[place]},
                device_id_type=MESH,
            )

    for table in tables:
        table.wait()

    def find_wanted(place):
        asker = jnp.clip(shard + OFFSETS[place], 0, shards - 1)
        bits = jnp.int32(0)
        for row in range(tiles_dev):
            live = counts[asker * tiles_dev + row]
            for pick in range(picks):
                tile = select[pick, asker * tiles_dev + row]
                wanted = (pick < live) & (tile // tiles_dev == shard)
                bits |= jnp.where(wanted, 1 << tile % tiles_dev, 0)
        first = lowest_bit(bits)
        send_bits[2 * place] = first
        send_bits[2 * place + 1] = lowest_bit(bits ^ first)

    def stage(head, some):
        for which in range(2):
            tiles = [own[head, which, tile * TILE : (tile + 1) * TILE] for tile in range(tiles_dev)]
            for place in some:
                for slot in range(CAP):
                    bit = send_bits[2 * place + slot]
                    chosen = tiles[-1]
                    for tile in range(tiles_dev - 1):
                        chosen = jnp.where(bit == 1 << tile, tiles[tile], chosen)
                    row = (which * CAP + slot) * TILE
                    staged[head, place, row : row + TILE] = chosen

    def await_tiles(head):
        for which in range(2):
            load(head, which).wait()

    def start_early(head, some=places):
        for place in some:
            there = inside(place, 1) & earlier(place)
            behind = crosses(place) if OFFSETS[place] == REACH else jnp.bool_(False)
            at = jnp.where(behind & (spot == row_shards - 1), head - LAG, head)

            @pl.when(there & (at >= 0) & (at < heads))
            def _():
                send(at, place).start()

    for place in reversed(places):
        find_wanted(place)
        if place == len(OFFSETS) - 1:
            await_tiles(0)
        stage(0, [place])
        start_early(0, [place])

    first_tile = (shard - REACH) * tiles_dev
    row_bits = []
    for row in range(tiles_dev):
        live = counts[shard * tiles_dev + row]
        bits = jnp.int32(0)
        for pick in range(picks):
            tile = select[pick, shard * tiles_dev + row] - first_tile
            bits |= jnp.where(pick < live, 1 << (tile & 31), 0)
        row_bits.append(bits)
    union = row_bits[0]
    for bits in row_bits[1:]:
        union |= bits
    pool_bits = [1 << (REACH * tiles_dev + tile) for tile in range(tiles_dev)]
    for place in places:
        base = (REACH - OFFSETS[place]) * tiles_dev
        block = union & (((1 << tiles_dev) - 1) << base)
        first = lowest_bit(block)
        pool_bits += [first, lowest_bit(block ^ first)]
    pool_tiles = len(pool_bits)
    for row in range(tiles_dev):
        for slot, bit in enumerate(pool_bits):
            bias[row * pool_tiles + slot] = jnp.where(
                (row_bits[row] & bit) != 0, jnp.float32(0), jnp.float32(-jnp.inf)
            )


    for place in places:

        @pl.when(jnp.logical_not(inside(place, -1)))
        def _():
            def clear(head, carry):
                pool[head, place] = jnp.zeros(pool.shape[2:], pool.dtype)
                return carry

            lax.fori_loop(0, heads, clear, 0)

    def fill(head, carry):
        await_tiles(head)
        stage(head, places)
        start_early(head)
        return carry

    lax.fori_loop(1, heads, fill, 0)
    for extra in range(LAG):
        start_early(heads + extra)

    for ahead in (True, False):
        some = [place for place in places if (OFFSETS[place] > 0) == ahead]
        later = [inside(place, 1) & jnp.logical_not(earlier(place)) for place in some]
        for place, there in zip(some, later):

            @pl.when(there)
            def _():
                pl.semaphore_wait(ready.at[place], 1)

        def start_later(head, carry):
            for place, there in zip(some, later):

                @pl.when(there)
                def _():
                    send(head, place).start()

            return carry

        lax.fori_loop(0, heads, start_later, 0)

    factor = HEAD_DIM ** (-0.5) * LOG2E
    across = (((1,), (1,)), ((), ()))

    def attend(head, side):
        rows = pl.multiple_of(side * half_rows, half_rows)
        query = queries[head, pl.ds(rows, half_rows)]
        raw = [lax.dot_general(query, own[head, 0], across, preferred_element_type=jnp.float32)]
        for place in places:
            raw.append(
                lax.dot_general(
                    query,
                    pool[head, place, : CAP * TILE],
                    across,
                    preferred_element_type=jnp.float32,
                )
            )
        blocks = []
        for block in raw:
            blocks += [block[:, at : at + TILE] for at in range(0, block.shape[1], TILE)]
        parts = []
        for part in range(half_rows // TILE):
            row = side * (half_rows // TILE) + part
            scores = [
                block[part * TILE : (part + 1) * TILE] + bias[row * pool_tiles + slot]
                for slot, block in enumerate(blocks)
            ]
            peak = scores[0]
            for score in scores[1:]:
                peak = jnp.maximum(peak, score)
            peak = jnp.max(peak, axis=1, keepdims=True)
            weights = [jnp.exp2((score - peak) * factor) for score in scores]
            total = weights[0]
            for weight in weights[1:]:
                total = total + weight
            total = jnp.sum(total, axis=1, keepdims=True)
            weights = [weight.astype(jnp.bfloat16) for weight in weights]
            parts.append((weights, total))
        stacked = [
            jnp.concatenate([weights[slot] for weights, _ in parts], axis=0)
            for slot in range(pool_tiles)
        ]
        totals = jnp.concatenate([total for _, total in parts], axis=0)
        update = jnp.dot(
            jnp.concatenate(stacked[:tiles_dev], axis=1),
            own[head, 1],
            preferred_element_type=jnp.float32,
        )
        for place in places:
            at = tiles_dev + CAP * place
            update += jnp.dot(
                jnp.concatenate(stacked[at : at + CAP], axis=1),
                pool[head, place, CAP * TILE :],
                preferred_element_type=jnp.float32,
            )
        branch_out[head, pl.ds(rows, half_rows)] = (update / totals).astype(jnp.bfloat16)

    guidance = guide_scale[0]

    def combine(head):
        swap(head).wait_recv()
        rows = pl.multiple_of(half * half_rows, half_rows)
        mine = branch_out[head, pl.ds(rows, half_rows)].astype(jnp.float32)
        other = theirs[head].astype(jnp.float32)
        cond_out = jnp.where(half == 0, mine, other)
        uncond = jnp.where(half == 0, other, mine)
        mixed = uncond + guidance * (cond_out - uncond)
        out[:, columns(head)] = mixed.astype(out.dtype)

    def step(head, carry):
        @pl.when(head > 0)
        def _():
            combine(head - 1)

        load(head, 2).wait()
        for place in places:

            @pl.when(inside(place, -1))
            def _():
                send(head, place).wait_recv()

        attend(head, 1 - half)
        swap(head).start()
        attend(head, half)

        return carry

    lax.fori_loop(0, heads, step, 0)

    def finish(head, carry):
        for place in places:

            @pl.when(inside(place, 1))
            def _():
                send(head, place).wait_send()

        return carry

    lax.fori_loop(0, heads, finish, 0)
    combine(heads - 1)

    def finish_swap(head, carry):
        swap(head).wait_send()
        return carry

    lax.fori_loop(0, heads, finish_swap, 0)


def body(row_shards, query_rows, key_rows, value_rows, select, counts, guide_scale):
    tokens, width = query_rows.shape
    heads = width // HEAD_DIM
    tiles_dev = tokens // TILE
    half_rows = tokens // 2
    places = len(OFFSETS)
    pool_tiles = tiles_dev + places * CAP
    kind = query_rows.dtype
    hbm = pl.BlockSpec(memory_space=pltpu.HBM)
    sent = (heads, places, 2 * CAP * TILE, HEAD_DIM)
    operands = [
        pltpu.with_memory_space_constraint(operand, pltpu.HBM)
        for operand in (query_rows, key_rows, value_rows, select.T, counts)
    ]
    return pl.pallas_call(
        functools.partial(kernel, row_shards),
        out_shape=pltpu.VMEM((half_rows, width), kind),
        in_specs=[hbm] * 5 + [pl.BlockSpec(memory_space=pltpu.SMEM)],
        out_specs=pl.BlockSpec(memory_space=pltpu.VMEM),
        scratch_shapes=[
            pltpu.VMEM((heads, tokens, HEAD_DIM), kind),
            pltpu.VMEM((heads, 2, tokens, HEAD_DIM), kind),
            pltpu.VMEM(sent, kind),
            pltpu.VMEM(sent, kind),
            pltpu.VMEM((heads, tokens, HEAD_DIM), kind),
            pltpu.VMEM((heads, half_rows, HEAD_DIM), kind),
            pltpu.SMEM(select.shape[::-1], select.dtype),
            pltpu.SMEM(counts.shape, counts.dtype),
            pltpu.SMEM((tiles_dev * pool_tiles,), jnp.float32),
            pltpu.SMEM((places * CAP,), jnp.int32),
            pltpu.SemaphoreType.DMA((heads, 3)),
            pltpu.SemaphoreType.DMA((heads, places)),
            pltpu.SemaphoreType.DMA((heads, places)),
            pltpu.SemaphoreType.DMA((heads,)),
            pltpu.SemaphoreType.DMA((heads,)),
            pltpu.SemaphoreType.DMA((2,)),
            pltpu.SemaphoreType.REGULAR((places,)),
        ],
        compiler_params=pltpu.CompilerParams(
            collective_id=0, has_side_effects=True, vmem_limit_bytes=48 * 1024 * 1024
        ),
        name="sparse_attention",
    )(*operands, guide_scale)


def solution(mesh):
    rows = P(("groups", "seq"), None)
    row_shards = len({device.coords[1] for device in mesh.devices.flat})
    local = functools.partial(body, row_shards)
    in_specs = (rows, rows, rows, P("groups", None), P("groups"), P("groups"))
    return jax.shard_map(local, mesh=mesh, in_specs=in_specs, out_specs=rows, check_vma=False)
```
